32 devices in a mesh: row: 4 (over y, x), col: 8 (over z, core).
Axes of the slice: x: 2, y: 2, z: 4, core: 2. Of those that a mesh axis runs over, the one named last changes fastest.
Arguments:
- wrapped: float32 [1, 4096, 8192], P(None, 'row', 'col'), may hold values from -2.8 to 2.8
- col_steps: int32 [1, 4, 8], P(None, 'row', 'col'), may hold values from -2 to 2, as said below
- row_steps: int32 [1, 4, 8], P(None, 'row', 'col'), may hold values from -2 to 2, as said below
Outputs:
- unwrapped: float32 [1, 4096, 8192], P(None, 'row', 'col')
The draws below stay inside these ranges and needn't reach their ends.
Inputs may be any that keep to these rules, and one draw needn't show every extreme that they name: `col_steps`: nonzero whole numbers; the last tile column has no edge. `row_steps`: nonzero whole numbers; the last tile row has no edge.
All inputs are finite; a program needn't handle non-finite values.
Results may differ from the reference program's by a relative error of at most 0.0003.
Values sent between devices are 32-bit elements; how exact they have to be, the bound alone decides.
A program may use at most 64 MiB of HBM per device.

```python
import math
import jax
import jax.numpy as jnp
from jax import lax

FRAMES = 1
TILE_ROWS = 1024
TILE_COLS = 1024
ITERS = 2
IMAGE_ROWS = 4096
IMAGE_COLS = 8192
N_ROW = 4
N_COL = 8


TWO_PI = 2.0 * math.pi


def draw_wrapped(key, part):
    extent = (FRAMES, IMAGE_ROWS, IMAGE_COLS)
    levels = jax.random.randint(jax.random.fold_in(key, 1), extent, -3, 4)
    speckle = jax.random.randint(jax.random.fold_in(key, 2), extent, 0, 5)
    levels = jnp.where(speckle == 0, levels, 0)
    jitter = jnp.clip(0.04 * jax.random.normal(jax.random.fold_in(key, 3), extent, jnp.float32), -0.1, 0.1)
    return (TWO_PI / 7.0 * levels.astype(jnp.float32) + jitter).astype(jnp.float32)


def signed_steps(key):
    extent = (FRAMES, N_ROW, N_COL)
    magnitude = jax.random.randint(jax.random.fold_in(key, 1), extent, 1, 3)
    polarity = 2 * jax.random.randint(jax.random.fold_in(key, 2), extent, 0, 2) - 1
    return (magnitude * polarity).astype(jnp.int32)


def draw_col_steps(key, part):
    return signed_steps(jax.random.fold_in(key, 11))


def draw_row_steps(key, part):
    return signed_steps(jax.random.fold_in(key, 12))


def setup_inputs(seed: int = 0) -> dict:
    arg_keys = jax.random.split(jax.random.key(seed), 4)
    return {
        "wrapped": draw_wrapped(jax.random.fold_in(arg_keys[3], 71), 0),
        "col_steps": draw_col_steps(jax.random.fold_in(arg_keys[3], 71), 0),
        "row_steps": draw_row_steps(jax.random.fold_in(arg_keys[3], 71), 0),
    }


TWO_PI = 2.0 * math.pi


def wrap_diff(change):
    return change - TWO_PI * jnp.floor(change / TWO_PI + 0.5)


def unwrap_frame(inputs):
    wrapped, col_steps, row_steps = inputs
    grid_x = wrap_diff(wrapped[:, 1:] - wrapped[:, :-1])
    grid_x = jnp.concatenate([grid_x, jnp.zeros((IMAGE_ROWS, 1), grid_x.dtype)], axis=1)
    grid_y = wrap_diff(wrapped[1:, :] - wrapped[:-1, :])
    grid_y = jnp.concatenate([grid_y, jnp.zeros((1, IMAGE_COLS), grid_y.dtype)], axis=0)
    charge = (grid_x[:-1, :-1] + grid_y[:-1, 1:] - grid_x[1:, :-1] - grid_y[:-1, :-1]) / TWO_PI
    charge = jnp.pad(charge, ((1, 0), (1, 0)))
    weight = 1.0 / (1.0 + jnp.abs(charge))
    tiled_shape = (N_ROW, TILE_ROWS, N_COL, TILE_COLS)
    step_x = grid_x.reshape(tiled_shape)
    step_y = grid_y.reshape(tiled_shape)
    weight_tiles = weight.reshape(tiled_shape)
    along_cols = jnp.cumsum(step_x, axis=3) - step_x
    first_column = step_y[:, :, :, 0]
    downward = jnp.cumsum(first_column, axis=1) - first_column
    anchor = wrapped.reshape(tiled_shape)[:, 0, :, 0]
    current = (anchor[:, None, :] + downward)[:, :, :, None] + along_cols
    col_weight = weight_tiles[:, :, :, -1]
    cross_x = step_x[:, :, :, -1]
    row_weight = weight_tiles[:, -1, :, :]
    cross_y = step_y[:, -1, :, :]
    cycles_across = TWO_PI * col_steps.astype(jnp.float32)
    cycles_down = TWO_PI * row_steps.astype(jnp.float32)
    for sweep in range(ITERS):
        beyond_x = jnp.concatenate([current[:, :, 1:, 0], jnp.zeros((N_ROW, TILE_ROWS, 1), current.dtype)], axis=2)
        horizontal = jnp.sum(col_weight * (current[:, :, :, -1] + cross_x - beyond_x), axis=1) / jnp.sum(col_weight, axis=1)
        beyond_y = jnp.concatenate([current[1:, 0, :, :], jnp.zeros((1, N_COL, TILE_COLS), current.dtype)], axis=0)
        vertical = jnp.sum(row_weight * (current[:, -1, :, :] + cross_y - beyond_y), axis=2) / jnp.sum(row_weight, axis=2)
        horizontal = horizontal + cycles_across
        vertical = vertical + cycles_down
        prefix_across = jnp.cumsum(horizontal, axis=1) - horizontal
        prefix_down = jnp.cumsum(vertical, axis=0) - vertical
        offset = 0.5 * (prefix_across + prefix_across[0:1, :] + prefix_down + prefix_down[:, 0:1])
        current = current + offset[:, None, :, None]
    return (current / TWO_PI).reshape(IMAGE_ROWS, IMAGE_COLS)


def reference(wrapped, col_steps, row_steps):
    return lax.map(unwrap_frame, (wrapped, col_steps, row_steps))
```

```python
import functools
import math

import jax
import jax.numpy as jnp
from jax import lax
from jax.experimental import pallas as pl
from jax.experimental.pallas import tpu as pltpu
from jax.sharding import PartitionSpec as P

ITERS = 2
PI = float(jnp.float32(math.pi))
TWO_PI = 2.0 * math.pi
MESH = pl.DeviceIdType.MESH
LANES = 128


def cycles(change):
    return jnp.where(change >= PI, 1.0, jnp.where(change < -PI, -1.0, 0.0))


def iota(shape, dim):
    return lax.broadcasted_iota(jnp.int32, shape, dim)


def total(values):
    return jnp.sum(values, axis=1, keepdims=True)


def shifted_in(values, first):
    lane = iota(values.shape, 1)
    return jnp.where(lane == 0, first, pltpu.roll(values, 1, 1))


def exclusive(values, dim, count):
    where = iota(values.shape, dim)
    running, reach = values, 1
    while reach < count:
        running = running + jnp.where(where >= reach, pltpu.roll(running, reach, dim), 0.0)
        reach *= 2
    return running - values


def edge_kernel(
    names, sizes, rows_step, cols_step,
    wrapped, col_steps, row_steps,
    integ, offset,
    cells, left_out, up_out, right_in, below_in, corner_above, corner_left,
    last_row, mine_out, every,
    load_sem, send_sem, recv_sem, gather_send, gather_recv,
):
    row_name, col_name = names
    grid_rows, grid_cols = sizes
    devices = grid_rows * grid_cols
    tile_rows, tile_cols = cells.shape
    my_row, my_col = lax.axis_index(row_name), lax.axis_index(col_name)
    me = my_row * grid_cols + my_col

    chunks = tile_rows // rows_step
    loads = []
    for q in range(chunks):
        span = pl.ds(q * rows_step, rows_step)
        copy = pltpu.make_async_copy(wrapped.at[span], cells.at[span], load_sem.at[q])
        copy.start()
        loads.append(copy)

    def peer_of(p):
        peer = lax.rem(me + p, devices)
        return peer, (peer // grid_cols, lax.rem(peer, grid_cols))

    barrier = pltpu.get_barrier_semaphore()

    def greet(p, carry):
        _, place = peer_of(p)
        pl.semaphore_signal(barrier, inc=1, device_id=place, device_id_type=MESH)
        return carry

    lax.fori_loop(1, devices, greet, 0)

    upper = (iota((cols_step, cols_step), 0) <= iota((cols_step, cols_step), 1)).astype(
        jnp.float32).astype(jnp.bfloat16)
    lower = (iota((rows_step, rows_step), 1) <= iota((rows_step, rows_step), 0)).astype(
        jnp.float32).astype(jnp.bfloat16)
    lane = iota((rows_step, LANES), 1)
    down_carry = jnp.zeros((1, LANES), jnp.float32)
    ends, firsts = [], []
    for q in range(chunks):
        loads[q].wait()
        rows = pl.ds(q * rows_step, rows_step)
        head = cells[rows, 0:LANES]
        above = cells[0:1, 0:LANES] if q == 0 else cells[q * rows_step - 1 : q * rows_step, 0:LANES]
        before = jnp.where(iota(head.shape, 0) == 0, above, pltpu.roll(head, 1, 0))
        down = down_carry + jnp.dot(
            lower, cycles(head - before).astype(jnp.bfloat16), preferred_element_type=jnp.float32
        )
        down_carry = down[rows_step - 1 : rows_step, :]
        carry = down[:, 0:1]
        firsts.append(jnp.where(lane == 0, head, carry).T[0:2, :])
        here = cells[rows, :]
        across = cycles(here - pltpu.roll(here, 1, 1))
        across = jnp.where(iota(here.shape, 1) == 0, 0.0, across).astype(jnp.bfloat16)
        for b in range(tile_cols // cols_step):
            cols = slice(b * cols_step, (b + 1) * cols_step)
            count = carry + jnp.dot(across[:, cols], upper, preferred_element_type=jnp.float32)
            carry = count[:, cols_step - 1 : cols_step]
            integ[rows, cols] = here[:, cols] * (1.0 / TWO_PI) - count
            if q == 0:
                up_out[1:2, cols] = count[0:1, :]
            if q == chunks - 1:
                last_row[0:1, cols] = count[rows_step - 1 : rows_step, :]
        if q == 0:
            up_out[0:1, :] = here[0:1, :]
        tail = here[:, tile_cols - LANES :]
        ends.append(jnp.where(lane == 0, carry, tail).T)
    for q in range(chunks):
        left_out[:, q * rows_step : (q + 1) * rows_step] = firsts[q]

    pl.semaphore_wait(barrier, devices - 1)
    corner = cells.at[pl.ds(tile_rows - 8, 8), pl.ds(tile_cols - LANES, LANES)]
    links = (
        (left_out, right_in, 0, -1, my_col > 0, my_col < grid_cols - 1),
        (up_out, below_in, -1, 0, my_row > 0, my_row < grid_rows - 1),
        (corner, corner_left, 0, 1, my_col < grid_cols - 1, my_col > 0),
        (corner, corner_above, 1, 0, my_row < grid_rows - 1, my_row > 0),
    )

    def link_copy(k, away):
        source, target, d_row, d_col, _, _ = links[k]
        place = (
            lax.rem(my_row + d_row * away + grid_rows, grid_rows),
            lax.rem(my_col + d_col * away + grid_cols, grid_cols),
        )
        return pltpu.make_async_remote_copy(
            src_ref=source, dst_ref=target, send_sem=send_sem.at[k], recv_sem=recv_sem.at[k],
            device_id=place, device_id_type=MESH,
        )

    for k in range(4):
        sends, receives = links[k][4], links[k][5]

        @pl.when(sends)
        def _():
            link_copy(k, 1).start()

        @pl.when(jnp.logical_not(receives))
        def _():
            target = links[k][1]
            target[...] = jnp.zeros(target.shape, jnp.float32)

    end_count = jnp.concatenate([e[0:1, :] for e in ends], axis=1)
    end_inner = jnp.concatenate([e[LANES - 2 : LANES - 1, :] for e in ends], axis=1)
    end_outer = jnp.concatenate([e[LANES - 1 : LANES, :] for e in ends], axis=1)
    row_inner = cells[tile_rows - 2 : tile_rows - 1, :]
    row_outer = cells[tile_rows - 1 : tile_rows, :]

    for k in range(4):

        @pl.when(links[k][5])
        def _():
            link_copy(k, 1).wait_recv()

    def base(inner, outer, inner_before, outer_before, at_image_edge, first, count, beyond):
        over = cycles(outer - inner)
        over_before = shifted_in(over, cycles(outer_before - inner_before))
        along_outer = cycles(outer - shifted_in(outer, outer_before))
        along_inner = cycles(inner - shifted_in(inner, inner_before))
        charge = over_before + along_outer - over - along_inner
        charge = jnp.where((iota(charge.shape, 1) == 0) & at_image_edge, 0.0, charge)
        weight = 1.0 / (1.0 + jnp.abs(charge))
        jump = beyond - count - cycles(first - outer)
        return total(weight * jump) / total(weight)

    across_base = base(
        end_inner, end_outer,
        corner_above[7:8, LANES - 2 : LANES - 1], corner_above[7:8, LANES - 1 : LANES],
        my_row == 0, right_in[0:1, :], end_count, right_in[1:2, :],
    ) + col_steps[0, 0].astype(jnp.float32)
    down_base = base(
        row_inner, row_outer,
        corner_left[6:7, LANES - 1 : LANES], corner_left[7:8, LANES - 1 : LANES],
        my_col == 0, below_in[0:1, :], last_row[...], below_in[1:2, :],
    ) + row_steps[0, 0].astype(jnp.float32)
    slot = iota((1, LANES), 1)
    mine_out[...] = jnp.where(
        slot == my_col, across_base, jnp.where(slot == grid_cols + my_col, down_base, 0.0)
    )

    def gather_copy(p, owner):
        _, place = peer_of(p)
        return pltpu.make_async_remote_copy(
            src_ref=mine_out, dst_ref=every.at[owner], send_sem=gather_send.at[p],
            recv_sem=gather_recv.at[owner], device_id=place, device_id_type=MESH,
        )

    def tell(p, carry):
        gather_copy(p, me).start()
        return carry

    def hear(p, carry):
        gather_copy(p, peer_of(p)[0]).wait_recv()
        return carry

    def sent(p, carry):
        gather_copy(p, me).wait_send()
        return carry

    lax.fori_loop(1, devices, tell, 0)
    every[pl.ds(me, 1)] = mine_out[...][None]
    lax.fori_loop(1, devices, hear, 0)

    padded = -(-grid_rows // 8) * 8
    tile_row = iota((padded, LANES), 0)
    tile_lane = iota((padded, LANES), 1)
    grid = jnp.zeros((padded, LANES), jnp.float32)
    for r in range(grid_rows):
        line = every[r * grid_cols]
        for c in range(1, grid_cols):
            line = line + every[r * grid_cols + c]
        grid = jnp.where(tile_row == r, line, grid)
    inside = tile_lane < grid_cols
    horizontal_base = jnp.where(inside, grid, 0.0)
    vertical_base = jnp.where(inside, pltpu.roll(grid, LANES - grid_cols, 1), 0.0)
    totals = jnp.zeros((padded, LANES), jnp.float32)
    for sweep in range(ITERS):
        right = jnp.where(tile_lane < grid_cols - 1, pltpu.roll(totals, LANES - 1, 1), 0.0)
        below = jnp.where(tile_row < grid_rows - 1, pltpu.roll(totals, padded - 1, 0), 0.0)
        horizontal = horizontal_base + totals - right
        vertical = vertical_base + totals - below
        prefix_across = exclusive(horizontal, 1, grid_cols)
        prefix_down = exclusive(vertical, 0, grid_rows)
        totals = totals + 0.5 * (
            prefix_across + prefix_across[0:1, :] + prefix_down + prefix_down[:, 0:1]
        )
    chosen = jnp.where((tile_row == my_row) & (tile_lane == my_col), totals, 0.0)
    mine = jnp.sum(jnp.sum(chosen, axis=1, keepdims=True), axis=0, keepdims=True)
    offset[...] = jnp.broadcast_to(mine, offset.shape)

    lax.fori_loop(1, devices, sent, 0)
    for k in range(4):

        @pl.when(links[k][4])
        def _():
            link_copy(k, 1).wait_send()


def on_device(names, sizes, wrapped, col_steps, row_steps):
    frames, tile_rows, tile_cols = wrapped.shape
    devices = sizes[0] * sizes[1]
    rows_step = math.gcd(tile_rows, 256)
    cols_step = math.gcd(tile_cols, 256)
    f32 = jnp.float32
    call = pl.pallas_call(
        functools.partial(edge_kernel, names, sizes, rows_step, cols_step),
        out_shape=(
            pltpu.VMEM((tile_rows, tile_cols), f32),
            jax.ShapeDtypeStruct((8, LANES), f32),
        ),
        in_specs=[
            pl.BlockSpec(memory_space=pltpu.HBM),
            pl.BlockSpec(memory_space=pltpu.SMEM),
            pl.BlockSpec(memory_space=pltpu.SMEM),
        ],
        out_specs=(
            pl.BlockSpec(memory_space=pltpu.VMEM),
            pl.BlockSpec(memory_space=pltpu.VMEM),
        ),
        scratch_shapes=[
            pltpu.VMEM((tile_rows, tile_cols), f32),
            pltpu.VMEM((2, tile_rows), f32),
            pltpu.VMEM((2, tile_cols), f32),
            pltpu.VMEM((2, tile_rows), f32),
            pltpu.VMEM((2, tile_cols), f32),
            pltpu.VMEM((8, LANES), f32),
            pltpu.VMEM((8, LANES), f32),
            pltpu.VMEM((1, tile_cols), f32),
            pltpu.VMEM((1, LANES), f32),
            pltpu.VMEM((devices, 1, LANES), f32),
            pltpu.SemaphoreType.DMA((tile_rows // rows_step,)),
            pltpu.SemaphoreType.DMA((4,)),
            pltpu.SemaphoreType.DMA((4,)),
            pltpu.SemaphoreType.DMA((devices,)),
            pltpu.SemaphoreType.DMA((devices,)),
        ],
        compiler_params=pltpu.CompilerParams(
            collective_id=0, has_side_effects=True, vmem_limit_bytes=24 * 1024 * 1024
        ),
    )
    outs = []
    for f in range(frames):
        integ, offset = call(wrapped[f], col_steps[f], row_steps[f])
        outs.append(integ + offset[0, 0])
    return jnp.stack(outs)


def solution(mesh):
    spec = P(None, "row", "col")
    sizes = (mesh.shape["row"], mesh.shape["col"])
    return jax.shard_map(
        functools.partial(on_device, ("row", "col"), sizes),
        mesh=mesh, in_specs=(spec, spec, spec), out_specs=spec, check_vma=False,
    )
```

```python
import functools
import math

import jax
import jax.numpy as jnp
from jax import lax
from jax.experimental import pallas as pl
from jax.experimental.pallas import tpu as pltpu
from jax.sharding import PartitionSpec as P

ITERS = 2
PI = float(jnp.float32(math.pi))
TWO_PI = 2.0 * math.pi
MESH = pl.DeviceIdType.MESH
LANES = 128


def cycles(change):
    return jnp.where(change >= PI, 1.0, jnp.where(change < -PI, -1.0, 0.0))


def iota(shape, dim):
    return lax.broadcasted_iota(jnp.int32, shape, dim)


def total(values):
    return jnp.sum(values, axis=1, keepdims=True)


def shifted_in(values, first):
    lane = iota(values.shape, 1)
    return jnp.where(lane == 0, first, pltpu.roll(values, 1, 1))


def exclusive(values, dim, count):
    where = iota(values.shape, dim)
    running, reach = values, 1
    while reach < count:
        running = running + jnp.where(where >= reach, pltpu.roll(running, reach, dim), 0.0)
        reach *= 2
    return running - values


def edge_kernel(
    names, sizes, rows_step, cols_step,
    wrapped, col_steps, row_steps,
    integ, offset,
    cells, left_out, up_out, right_in, below_in, corner_above, corner_left,
    last_row, end_lines, down, floors, mine_out, every,
    load_sem, send_sem, recv_sem, gather_send, gather_recv, all_in,
):
    row_name, col_name = names
    grid_rows, grid_cols = sizes
    devices = grid_rows * grid_cols
    tile_rows, tile_cols = cells.shape
    my_row, my_col = lax.axis_index(row_name), lax.axis_index(col_name)
    me = my_row * grid_cols + my_col

    chunks = tile_rows // rows_step
    rest = pl.ds(LANES, tile_cols - LANES)
    regions = [(pl.ds(0, tile_rows), pl.ds(0, LANES)), (pl.ds(0, 16), rest)]
    for q in range(chunks):
        top = max(q * rows_step, 16)
        regions.append((pl.ds(top, (q + 1) * rows_step - top), rest))
    loads = []
    for k, (rows, cols) in enumerate(regions):
        loads.append(
            pltpu.make_async_copy(wrapped.at[0, rows, cols], cells.at[rows, cols], load_sem.at[k])
        )
        loads[-1].start()

    def row_place(p):
        return my_row, lax.rem(my_col + p, grid_cols)

    def col_place(p):
        return lax.rem(my_row + p, grid_rows), my_col

    def signal_all(semaphore, place, count):
        def signal(p, carry):
            pl.semaphore_signal(semaphore, inc=1, device_id=place(p), device_id_type=MESH)
            return carry

        lax.fori_loop(1, count, signal, 0)

    barrier = pltpu.get_barrier_semaphore()
    signal_all(barrier, col_place, grid_rows)
    signal_all(barrier, row_place, grid_cols)

    def peer_of(p):
        peer = lax.rem(me + p, devices)
        return peer, (peer // grid_cols, lax.rem(peer, grid_cols))

    def triangle(size, dim):
        ordered = iota((size, size), dim) <= iota((size, size), 1 - dim)
        return ordered.astype(jnp.float32).astype(jnp.bfloat16)

    upper, lower = triangle(cols_step, 0), triangle(rows_step, 1)
    lane = iota((rows_step, LANES), 1)
    blocks = [slice(b * cols_step, (b + 1) * cols_step) for b in range(tile_cols // cols_step)]

    def along(rows, carry):
        for cols in blocks:
            count = carry + jnp.dot(floors[rows, cols], upper, preferred_element_type=jnp.float32)
            carry = count[:, cols_step - 1 : cols_step]
            yield cols, count

    down_carry = jnp.zeros((1, LANES), jnp.float32)
    with jax.named_scope("load_head"):
        loads[0].wait()
    with jax.named_scope("head"):
        for q in range(chunks):
            top = q * rows_step
            rows = pl.ds(top, rows_step)
            head = cells[rows, 0:LANES]
            above = cells[max(top - 1, 0) : max(top, 1), 0:LANES]
            before = jnp.where(iota(head.shape, 0) == 0, above, pltpu.roll(head, 1, 0))
            counts = down_carry + jnp.dot(
                lower, cycles(head - before).astype(jnp.bfloat16), preferred_element_type=jnp.float32
            )
            down_carry = counts[rows_step - 1 : rows_step, :]
            down[rows, :] = jnp.broadcast_to(counts[:, 0:1], (rows_step, LANES))
            left_out[:, top : top + rows_step] = jnp.where(lane == 0, head, counts[:, 0:1]).T[0:2, :]
    with jax.named_scope("load_top"):
        loads[1].wait()

    def set_floors(rows):
        here = cells[rows, :]
        across = cycles(here - pltpu.roll(here, 1, 1))
        across = jnp.where(iota(here.shape, 1) == 0, 0.0, across)
        floors[rows, :] = across.astype(jnp.bfloat16)
        return here, across

    with jax.named_scope("first_row"):
        set_floors(pl.ds(0, 16))
        up_out[0:1, :] = cells[0:1, :]
        for cols, count in along(pl.ds(0, 16), down[0:16, 0:1]):
            up_out[1:2, cols] = count[0:1, :]

    with jax.named_scope("barrier"):
        pl.semaphore_wait(barrier, grid_rows + grid_cols - 2)
    corner = cells.at[pl.ds(tile_rows - 8, 8), pl.ds(tile_cols - LANES, LANES)]
    links = (
        (left_out, right_in, 0, -1, my_col > 0, my_col < grid_cols - 1),
        (up_out, below_in, -1, 0, my_row > 0, my_row < grid_rows - 1),
        (corner, corner_left, 0, 1, my_col < grid_cols - 1, my_col > 0),
        (corner, corner_above, 1, 0, my_row < grid_rows - 1, my_row > 0),
    )

    def link_copy(k, away):
        source, target, d_row, d_col, _, _ = links[k]
        place = (
            lax.rem(my_row + d_row * away + grid_rows, grid_rows),
            lax.rem(my_col + d_col * away + grid_cols, grid_cols),
        )
        return pltpu.make_async_remote_copy(
            src_ref=source, dst_ref=target, send_sem=send_sem.at[k], recv_sem=recv_sem.at[k],
            device_id=place, device_id_type=MESH,
        )

    def launch(k):
        sends, receives = links[k][4], links[k][5]

        @pl.when(sends)
        def _():
            link_copy(k, 1).start()

        @pl.when(jnp.logical_not(receives))
        def _():
            target = links[k][1]
            target[...] = jnp.zeros(target.shape, jnp.float32)

    launch(0)
    launch(1)
    signal_all(all_in, col_place, grid_rows)
    for k in range(2, len(loads)):
        with jax.named_scope(f"load_{k}"):
            loads[k].wait()
    launch(2)
    launch(3)
    for q in range(chunks):
        top = q * rows_step
        rows = pl.ds(top, rows_step)
        with jax.named_scope(f"floors_{q}"):
            here, across = set_floors(rows)
            sums = across[:, 0:LANES]
            for j in range(1, tile_cols // LANES):
                sums = sums + across[:, j * LANES : (j + 1) * LANES]
            ends = down[rows, 0:1] + total(sums)
            tail = jnp.where(lane == 0, ends, here[:, tile_cols - LANES :]).T
            end_lines[0:1, top : top + rows_step] = tail[0:1, :]
            end_lines[1:3, top : top + rows_step] = tail[LANES - 2 :, :]

    with jax.named_scope("last_row"):
        for cols, count in along(pl.ds(tile_rows - 16, 16), down[tile_rows - 16 :, 0:1]):
            last_row[0:1, cols] = count[15:16, :]
    row_inner = cells[tile_rows - 2 : tile_rows - 1, :]
    row_outer = cells[tile_rows - 1 : tile_rows, :]

    for k in range(4):

        with jax.named_scope(f"halo_{k}"):

            @pl.when(links[k][5])
            def _():
                link_copy(k, 1).wait_recv()

    def base(inner, outer, inner_before, outer_before, at_image_edge, first, count, beyond):
        over = cycles(outer - inner)
        over_before = shifted_in(over, cycles(outer_before - inner_before))
        along_outer = cycles(outer - shifted_in(outer, outer_before))
        along_inner = cycles(inner - shifted_in(inner, inner_before))
        charge = over_before + along_outer - over - along_inner
        charge = jnp.where((iota(charge.shape, 1) == 0) & at_image_edge, 0.0, charge)
        weight = 1.0 / (1.0 + jnp.abs(charge))
        jump = beyond - count - cycles(first - outer)
        return total(weight * jump) / total(weight)

    across_base = base(
        end_lines[1:2, :], end_lines[2:3, :],
        corner_above[7:8, LANES - 2 : LANES - 1], corner_above[7:8, LANES - 1 : LANES],
        my_row == 0, right_in[0:1, :], end_lines[0:1, :], right_in[1:2, :],
    ) + col_steps[0].astype(jnp.float32)
    down_base = base(
        row_inner, row_outer,
        corner_left[6:7, LANES - 1 : LANES], corner_left[7:8, LANES - 1 : LANES],
        my_col == 0, below_in[0:1, :], last_row[...], below_in[1:2, :],
    ) + row_steps[0].astype(jnp.float32)
    slot = iota((1, LANES), 1)
    mine_out[...] = jnp.where(
        slot == my_col, across_base, jnp.where(slot == grid_cols + my_col, down_base, 0.0)
    )

    def gather_copy(p, owner):
        _, place = peer_of(p)
        return pltpu.make_async_remote_copy(
            src_ref=mine_out, dst_ref=every.at[owner], send_sem=gather_send.at[p],
            recv_sem=gather_recv.at[owner], device_id=place, device_id_type=MESH,
        )

    def tell(p, carry):
        gather_copy(p, me).start()
        return carry

    def hear(p, carry):
        gather_copy(p, peer_of(p)[0]).wait_recv()
        return carry

    def sent(p, carry):
        gather_copy(p, me).wait_send()
        return carry

    with jax.named_scope("all_in"):
        pl.semaphore_wait(all_in, grid_rows - 1)
    with jax.named_scope("tell"):
        lax.fori_loop(1, devices, tell, 0)
    every[pl.ds(me, 1)] = mine_out[...][None]
    with jax.named_scope("integrate"):
        for q in range(chunks):
            rows = pl.ds(q * rows_step, rows_step)
            for cols, count in along(rows, down[rows, 0:1]):
                integ[rows, cols] = cells[rows, cols] * (1.0 / TWO_PI) - count
    with jax.named_scope("sent"):
        lax.fori_loop(1, devices, sent, 0)
        for k in range(4):

            @pl.when(links[k][4])
            def _():
                link_copy(k, 1).wait_send()

    with jax.named_scope("hear"):
        lax.fori_loop(1, devices, hear, 0)

    padded = -(-grid_rows // 8) * 8
    tile_row = iota((padded, LANES), 0)
    tile_lane = iota((padded, LANES), 1)
    grid = jnp.zeros((padded, LANES), jnp.float32)
    for r in range(grid_rows):
        line = every[r * grid_cols]
        for c in range(1, grid_cols):
            line = line + every[r * grid_cols + c]
        grid = jnp.where(tile_row == r, line, grid)
    inside = tile_lane < grid_cols
    horizontal_base = jnp.where(inside, grid, 0.0)
    vertical_base = jnp.where(inside, pltpu.roll(grid, LANES - grid_cols, 1), 0.0)
    base_across = exclusive(horizontal_base, 1, grid_cols)
    base_down = exclusive(vertical_base, 0, grid_rows)
    totals = jnp.zeros((padded, LANES), jnp.float32)
    for sweep in range(ITERS):
        prefix_across = base_across + (totals[:, 0:1] - totals)
        prefix_down = base_down + (totals[0:1, :] - totals)
        totals = totals + 0.5 * (
            prefix_across + prefix_across[0:1, :] + prefix_down + prefix_down[:, 0:1]
        )
    chosen = jnp.where((tile_row == my_row) & (tile_lane == my_col), totals, 0.0)
    mine = jnp.sum(jnp.sum(chosen, axis=1, keepdims=True), axis=0, keepdims=True)
    offset[...] = jnp.broadcast_to(mine, offset.shape)


def place_kernel(integ, offset, out, ready, sems):
    parts = sems.shape[0]
    step = integ.shape[0] // parts
    shift = offset[0:1, 0:1]
    copies = []
    for q in range(parts):
        rows = pl.ds(q * step, step)
        ready[rows, :] = integ[rows, :] + shift
        copy = pltpu.make_async_copy(ready.at[rows], out.at[rows], sems.at[q])
        copy.start()
        copies.append(copy)
    for copy in copies:
        copy.wait()


def on_device(names, sizes, wrapped, col_steps, row_steps):
    frames, tile_rows, tile_cols = wrapped.shape
    devices = sizes[0] * sizes[1]
    rows_step = math.gcd(tile_rows, 256)
    cols_step = math.gcd(tile_cols, 256)
    f32 = jnp.float32
    call = pl.pallas_call(
        functools.partial(edge_kernel, names, sizes, rows_step, cols_step),
        out_shape=(
            pltpu.VMEM((tile_rows, tile_cols), f32),
            pltpu.VMEM((8, LANES), f32),
        ),
        in_specs=[
            pl.BlockSpec(memory_space=pltpu.HBM),
            pl.BlockSpec(memory_space=pltpu.VMEM),
            pl.BlockSpec(memory_space=pltpu.VMEM),
        ],
        out_specs=(
            pl.BlockSpec(memory_space=pltpu.VMEM),
            pl.BlockSpec(memory_space=pltpu.VMEM),
        ),
        scratch_shapes=[
            pltpu.VMEM((tile_rows, tile_cols), f32),
            pltpu.VMEM((2, tile_rows), f32),
            pltpu.VMEM((2, tile_cols), f32),
            pltpu.VMEM((2, tile_rows), f32),
            pltpu.VMEM((2, tile_cols), f32),
            pltpu.VMEM((8, LANES), f32),
            pltpu.VMEM((8, LANES), f32),
            pltpu.VMEM((1, tile_cols), f32),
            pltpu.VMEM((3, tile_rows), f32),
            pltpu.VMEM((tile_rows, LANES), f32),
            pltpu.VMEM((tile_rows, tile_cols), jnp.bfloat16),
            pltpu.VMEM((1, LANES), f32),
            pltpu.VMEM((devices, 1, LANES), f32),
            pltpu.SemaphoreType.DMA((tile_rows // rows_step + 2,)),
            pltpu.SemaphoreType.DMA((4,)),
            pltpu.SemaphoreType.DMA((4,)),
            pltpu.SemaphoreType.DMA((devices,)),
            pltpu.SemaphoreType.DMA((devices,)),
            pltpu.SemaphoreType.REGULAR,
        ],
        compiler_params=pltpu.CompilerParams(
            collective_id=0, has_side_effects=True, vmem_limit_bytes=57 * 1024 * 1024
        ),
    )
    parts = math.gcd(tile_rows // 8, 16)
    place = pl.pallas_call(
        place_kernel,
        out_shape=jax.ShapeDtypeStruct((tile_rows, tile_cols), f32),
        in_specs=[pl.BlockSpec(memory_space=pltpu.VMEM), pl.BlockSpec(memory_space=pltpu.VMEM)],
        out_specs=pl.BlockSpec(memory_space=pltpu.HBM),
        scratch_shapes=[
            pltpu.VMEM((tile_rows, tile_cols), f32),
            pltpu.SemaphoreType.DMA((parts,)),
        ],
        compiler_params=pltpu.CompilerParams(vmem_limit_bytes=24 * 1024 * 1024),
    )
    outs = [
        place(*call(wrapped[f : f + 1], col_steps[f : f + 1], row_steps[f : f + 1]))
        for f in range(frames)
    ]
    return jnp.stack(outs)


def solution(mesh):
    spec = P(None, "row", "col")
    sizes = (mesh.shape["row"], mesh.shape["col"])
    return jax.shard_map(
        functools.partial(on_device, ("row", "col"), sizes),
        mesh=mesh, in_specs=(spec, spec, spec), out_specs=spec, check_vma=False,
    )
```

```python
import functools
import math

import jax
import jax.numpy as jnp
from jax import lax
from jax.experimental import pallas as pl
from jax.experimental.pallas import tpu as pltpu
from jax.sharding import PartitionSpec as P

ITERS = 2
TWO_PI = 2.0 * math.pi
MESH = pl.DeviceIdType.MESH
LANES = 128
STRIP = 16


def cycles(change):
    return jnp.floor(change * (1.0 / TWO_PI) + 0.5)


def iota(shape, dim):
    return lax.broadcasted_iota(jnp.int32, shape, dim)


def total(values):
    return jnp.sum(values, axis=1, keepdims=True)


def shifted_in(values, first):
    lane = iota(values.shape, 1)
    return jnp.where(lane == 0, first, pltpu.roll(values, 1, 1))


def triangle(size, dim):
    ordered = iota((size, size), dim) <= iota((size, size), 1 - dim)
    return ordered.astype(jnp.float32).astype(jnp.bfloat16)


def line_counts(line, step):
    lane = iota(line.shape, 1)
    floors = jnp.where(lane == 0, 0.0, cycles(line - pltpu.roll(line, 1, 1)))
    floors = jnp.broadcast_to(floors, (16, line.shape[1]))
    upper, ones = triangle(step, 0), jnp.ones((step, step), jnp.bfloat16)
    earlier, counts = None, []
    for b in range(line.shape[1] // step):
        piece = floors[:, b * step : (b + 1) * step]
        count = jnp.dot(piece.astype(jnp.bfloat16), upper, preferred_element_type=jnp.float32)
        if b > 0:
            count = count + jnp.dot(
                earlier.astype(jnp.bfloat16), ones, preferred_element_type=jnp.float32
            )
        earlier = piece if b == 0 else earlier + piece
        counts.append(count[0:1, :])
    return jnp.concatenate(counts, axis=1)


def edge_kernel(
    names, sizes, rows_step, cols_step,
    wrapped, col_steps, row_steps,
    integ, offset,
    cells, left_out, up_out, right_in, below_in, corner_above, corner_left,
    last_row, end_lines, row_sums, floors, mine_out, every,
    load_sem, send_sem, recv_sem, gather_send, gather_recv, all_in,
):
    row_name, col_name = names
    grid_rows, grid_cols = sizes
    devices = grid_rows * grid_cols
    tile_rows, tile_cols = cells.shape
    my_row, my_col = lax.axis_index(row_name), lax.axis_index(col_name)
    me = my_row * grid_cols + my_col

    chunks = tile_rows // rows_step
    rest = pl.ds(LANES, tile_cols - LANES)
    regions = [(pl.ds(0, tile_rows), pl.ds(0, LANES)), (pl.ds(0, 16), rest)]
    for q in range(chunks):
        top = max(q * rows_step, 16)
        regions.append((pl.ds(top, (q + 1) * rows_step - top), rest))
    loads = []
    for k, (rows, cols) in enumerate(regions):
        loads.append(
            pltpu.make_async_copy(wrapped.at[0, rows, cols], cells.at[rows, cols], load_sem.at[k])
        )
        loads[-1].start()

    def row_place(p):
        return my_row, lax.rem(my_col + p, grid_cols)

    def col_place(p):
        return lax.rem(my_row + p, grid_rows), my_col

    def signal_all(semaphore, place, count):
        def signal(p, carry):
            pl.semaphore_signal(semaphore, inc=1, device_id=place(p), device_id_type=MESH)
            return carry

        lax.fori_loop(1, count, signal, 0)

    every[...] = jnp.zeros(every.shape, jnp.float32)

    barrier = pltpu.get_barrier_semaphore()
    signal_all(barrier, col_place, grid_rows)
    signal_all(barrier, row_place, grid_cols)

    with jax.named_scope("load_head"):
        loads[0].wait()
    with jax.named_scope("head"):
        for q in range(chunks):
            span = slice(q * rows_step, (q + 1) * rows_step)
            left_out[0:1, span] = cells[span, 0:LANES].T[0:1, :]
        left_out[1:2, :] = line_counts(left_out[0:1, :], rows_step)
    with jax.named_scope("load_top"):
        loads[1].wait()
    with jax.named_scope("first_row"):
        up_out[0:1, :] = cells[0:1, :]
        up_out[1:2, :] = line_counts(cells[0:1, :], cols_step)

    with jax.named_scope("barrier"):
        pl.semaphore_wait(barrier, grid_rows + grid_cols - 2)
    corner = cells.at[pl.ds(tile_rows - 8, 8), pl.ds(tile_cols - LANES, LANES)]
    links = (
        (left_out, right_in, 0, -1, my_col > 0, my_col < grid_cols - 1),
        (up_out, below_in, -1, 0, my_row > 0, my_row < grid_rows - 1),
        (corner, corner_left, 0, 1, my_col < grid_cols - 1, my_col > 0),
        (corner, corner_above, 1, 0, my_row < grid_rows - 1, my_row > 0),
    )

    def link_copy(k, away):
        source, target, d_row, d_col, _, _ = links[k]
        place = (
            lax.rem(my_row + d_row * away + grid_rows, grid_rows),
            lax.rem(my_col + d_col * away + grid_cols, grid_cols),
        )
        return pltpu.make_async_remote_copy(
            src_ref=source, dst_ref=target, send_sem=send_sem.at[k], recv_sem=recv_sem.at[k],
            device_id=place, device_id_type=MESH,
        )

    def launch(k):
        sends, receives = links[k][4], links[k][5]

        @pl.when(sends)
        def _():
            link_copy(k, 1).start()

        @pl.when(jnp.logical_not(receives))
        def _():
            target = links[k][1]
            target[...] = jnp.zeros(target.shape, jnp.float32)

    launch(0)
    launch(1)
    signal_all(all_in, col_place, grid_rows)
    lane = iota((STRIP, LANES), 1)

    def strip(k, carry):
        rows = pl.ds(pl.multiple_of(k * STRIP, STRIP), STRIP)
        wrapped_around = cells[rows, 0:LANES]
        sums = jnp.zeros((STRIP, LANES), jnp.float32)
        for j in range(tile_cols // LANES):
            cols = slice(j * LANES, (j + 1) * LANES)
            here = cells[rows, cols]
            rolled = pltpu.roll(here, 1, 1)
            across = cycles(here - jnp.where(lane == 0, wrapped_around, rolled))
            wrapped_around = rolled
            floors[rows, cols] = across.astype(jnp.bfloat16)
            sums = sums + across
        row_sums[rows, :] = sums.astype(jnp.bfloat16)
        return carry

    per_chunk = rows_step // STRIP
    for q in range(chunks):
        with jax.named_scope(f"load_{q}"):
            loads[q + 2].wait()
        if q == chunks - 1:
            launch(2)
            launch(3)
        with jax.named_scope(f"floors_{q}"):
            lax.fori_loop(q * per_chunk, (q + 1) * per_chunk, strip, 0, unroll=math.gcd(per_chunk, 8))
    with jax.named_scope("ends"):
        ones = jnp.ones((16, LANES), jnp.bfloat16)
        for q in range(chunks):
            span = slice(q * rows_step, (q + 1) * rows_step)
            sums = lax.dot_general(
                ones, row_sums[span, :], (((1,), (1,)), ((), ())),
                preferred_element_type=jnp.float32,
            )
            end_lines[0:1, span] = left_out[1:2, span] + sums[0:1, :]
            end_lines[1:3, span] = cells[span, tile_cols - LANES :].T[LANES - 2 :, :]
    with jax.named_scope("last_row"):
        last_row[...] = left_out[1:2, tile_rows - 1 :] + line_counts(
            cells[tile_rows - 1 : tile_rows, :], cols_step
        )
    row_inner = cells[tile_rows - 2 : tile_rows - 1, :]
    row_outer = cells[tile_rows - 1 : tile_rows, :]

    for k in range(4):

        with jax.named_scope(f"halo_{k}"):

            @pl.when(links[k][5])
            def _():
                link_copy(k, 1).wait_recv()

    def base(inner, outer, inner_before, outer_before, at_image_edge, first, count, beyond):
        over = cycles(outer - inner)
        over_before = shifted_in(over, cycles(outer_before - inner_before))
        along_outer = cycles(outer - shifted_in(outer, outer_before))
        along_inner = cycles(inner - shifted_in(inner, inner_before))
        charge = over_before + along_outer - over - along_inner
        charge = jnp.where((iota(charge.shape, 1) == 0) & at_image_edge, 0.0, charge)
        weight = 1.0 / (1.0 + jnp.abs(charge))
        jump = beyond - count - cycles(first - outer)
        return total(weight * jump) / total(weight)

    across_base = base(
        end_lines[1:2, :], end_lines[2:3, :],
        corner_above[7:8, LANES - 2 : LANES - 1], corner_above[7:8, LANES - 1 : LANES],
        my_row == 0, right_in[0:1, :], end_lines[0:1, :], right_in[1:2, :],
    ) + col_steps[0].astype(jnp.float32)
    down_base = base(
        row_inner, row_outer,
        corner_left[6:7, LANES - 1 : LANES], corner_left[7:8, LANES - 1 : LANES],
        my_col == 0, below_in[0:1, :], last_row[...], below_in[1:2, :],
    ) + row_steps[0].astype(jnp.float32)
    slot = iota((1, LANES), 1)
    mine_out[...] = jnp.where(
        slot == my_col, across_base, jnp.where(slot == grid_cols + my_col, down_base, 0.0)
    )

    def gather_copy(row, col, owner):
        peer = row * grid_cols + col
        return pltpu.make_async_remote_copy(
            src_ref=mine_out, dst_ref=every.at[owner], send_sem=gather_send.at[peer],
            recv_sem=gather_recv.at[owner], device_id=(row, col), device_id_type=MESH,
        )

    def span(low, high, act):
        def step(k, carry):
            act(k)
            return carry

        lax.fori_loop(low, high, step, 0)

    def each_target(act):
        first_row = jnp.where(my_row == 0, 1, jnp.where(my_col == 0, my_row + 1, grid_rows))
        span(first_row, grid_rows, lambda r: span(my_col + 1, grid_cols, lambda c: act(r, c)))
        span(my_col + 1, grid_cols, lambda c: act(my_row, c))
        span(my_row + 1, grid_rows, lambda r: act(r, my_col))

    def each_source(act):
        span(0, my_col, lambda c: act(my_row, c))
        span(0, my_row, lambda r: act(r, my_col))
        span(0, jnp.where(my_row > 0, my_col, 0), lambda c: act(0, c))
        span(1, jnp.where(my_col > 0, my_row, 0), lambda r: act(r, 0))

    with jax.named_scope("all_in"):
        pl.semaphore_wait(all_in, grid_rows - 1)
    with jax.named_scope("tell"):
        each_target(lambda r, c: gather_copy(r, c, me).start())
    with jax.named_scope("integrate"):
        upper, lower = triangle(cols_step, 0), triangle(rows_step, 1)
        down_carry = jnp.zeros((1, LANES), jnp.float32)
        for q in range(chunks):
            top = q * rows_step
            rows = pl.ds(top, rows_step)
            head = cells[rows, 0:LANES]
            above = cells[max(top - 1, 0) : max(top, 1), 0:LANES]
            before = jnp.where(iota(head.shape, 0) == 0, above, pltpu.roll(head, 1, 0))
            counts = down_carry + jnp.dot(
                lower, cycles(head - before).astype(jnp.bfloat16), preferred_element_type=jnp.float32
            )
            down_carry = counts[rows_step - 1 : rows_step, :]
            carry = counts[:, 0:1]
            for b in range(tile_cols // cols_step):
                cols = slice(b * cols_step, (b + 1) * cols_step)
                count = carry + jnp.dot(
                    floors[rows, cols], upper, preferred_element_type=jnp.float32
                )
                carry = count[:, cols_step - 1 : cols_step]
                integ[rows, cols] = cells[rows, cols] * (1.0 / TWO_PI) - count
    with jax.named_scope("sent"):
        each_target(lambda r, c: gather_copy(r, c, me).wait_send())
        for k in range(4):

            @pl.when(links[k][4])
            def _():
                link_copy(k, 1).wait_send()

    with jax.named_scope("hear"):
        each_source(lambda r, c: gather_copy(r, c, r * grid_cols + c).wait_recv())

    padded = -(-grid_rows // 8) * 8
    tile_row = iota((padded, LANES), 0)
    tile_lane = iota((padded, LANES), 1)
    grid = jnp.zeros((padded, LANES), jnp.float32)
    for r in range(grid_rows):
        line = every[r * grid_cols]
        for c in range(1, grid_cols):
            line = line + every[r * grid_cols + c]
        grid = jnp.where(tile_row == r, line, grid)
    def summed(mask):
        picked = jnp.where(mask, grid, 0.0)
        return jnp.sum(jnp.sum(picked, axis=0, keepdims=True), axis=1, keepdims=True)

    earlier_cols = tile_lane < my_col
    across_here = summed((tile_row == my_row) & earlier_cols)
    across_top = summed((tile_row == 0) & earlier_cols)
    down_here = summed((tile_row < my_row) & (tile_lane == grid_cols + my_col))
    down_left = summed((tile_row < my_row) & (tile_lane == grid_cols))
    here = left = top = origin = jnp.zeros((1, 1), jnp.float32)
    for sweep in range(ITERS):
        prefix_across = across_here + (left - here)
        prefix_across_top = across_top + (origin - top)
        prefix_down = down_here + (top - here)
        prefix_down_left = down_left + (origin - left)
        here = here + 0.5 * (prefix_across + prefix_across_top + prefix_down + prefix_down_left)
        left = left + prefix_down_left
        top = top + prefix_across_top
    offset[...] = jnp.broadcast_to(here, offset.shape)


def place_kernel(integ, offset, out, ready, sems):
    parts = sems.shape[0]
    step = integ.shape[0] // parts
    shift = offset[0:1, 0:1]
    copies = []
    for q in range(parts):
        rows = pl.ds(q * step, step)
        ready[rows, :] = integ[rows, :] + shift
        copy = pltpu.make_async_copy(ready.at[rows], out.at[rows], sems.at[q])
        copy.start()
        copies.append(copy)
    for copy in copies:
        copy.wait()


def on_device(names, sizes, wrapped, col_steps, row_steps):
    frames, tile_rows, tile_cols = wrapped.shape
    devices = sizes[0] * sizes[1]
    rows_step = math.gcd(tile_rows, 256)
    cols_step = math.gcd(tile_cols, 256)
    f32 = jnp.float32
    call = pl.pallas_call(
        functools.partial(edge_kernel, names, sizes, rows_step, cols_step),
        out_shape=(
            pltpu.VMEM((tile_rows, tile_cols), f32),
            pltpu.VMEM((8, LANES), f32),
        ),
        in_specs=[
            pl.BlockSpec(memory_space=pltpu.HBM),
            pl.BlockSpec(memory_space=pltpu.VMEM),
            pl.BlockSpec(memory_space=pltpu.VMEM),
        ],
        out_specs=(
            pl.BlockSpec(memory_space=pltpu.VMEM),
            pl.BlockSpec(memory_space=pltpu.VMEM),
        ),
        scratch_shapes=[
            pltpu.VMEM((tile_rows, tile_cols), f32),
            pltpu.VMEM((2, tile_rows), f32),
            pltpu.VMEM((2, tile_cols), f32),
            pltpu.VMEM((2, tile_rows), f32),
            pltpu.VMEM((2, tile_cols), f32),
            pltpu.VMEM((8, LANES), f32),
            pltpu.VMEM((8, LANES), f32),
            pltpu.VMEM((1, tile_cols), f32),
            pltpu.VMEM((3, tile_rows), f32),
            pltpu.VMEM((tile_rows, LANES), jnp.bfloat16),
            pltpu.VMEM((tile_rows, tile_cols), jnp.bfloat16),
            pltpu.VMEM((1, LANES), f32),
            pltpu.VMEM((devices, 1, LANES), f32),
            pltpu.SemaphoreType.DMA((tile_rows // rows_step + 2,)),
            pltpu.SemaphoreType.DMA((4,)),
            pltpu.SemaphoreType.DMA((4,)),
            pltpu.SemaphoreType.DMA((devices,)),
            pltpu.SemaphoreType.DMA((devices,)),
            pltpu.SemaphoreType.REGULAR,
        ],
        compiler_params=pltpu.CompilerParams(
            collective_id=0, has_side_effects=True, vmem_limit_bytes=57 * 1024 * 1024
        ),
    )
    parts = math.gcd(tile_rows // 8, 16)
    place = pl.pallas_call(
        place_kernel,
        out_shape=jax.ShapeDtypeStruct((tile_rows, tile_cols), f32),
        in_specs=[pl.BlockSpec(memory_space=pltpu.VMEM), pl.BlockSpec(memory_space=pltpu.VMEM)],
        out_specs=pl.BlockSpec(memory_space=pltpu.HBM),
        scratch_shapes=[
            pltpu.VMEM((tile_rows, tile_cols), f32),
            pltpu.SemaphoreType.DMA((parts,)),
        ],
        compiler_params=pltpu.CompilerParams(vmem_limit_bytes=24 * 1024 * 1024),
    )
    outs = [
        place(*call(wrapped[f : f + 1], col_steps[f : f + 1], row_steps[f : f + 1]))
        for f in range(frames)
    ]
    return jnp.stack(outs)


def solution(mesh):
    spec = P(None, "row", "col")
    sizes = (mesh.shape["row"], mesh.shape["col"])
    return jax.shard_map(
        functools.partial(on_device, ("row", "col"), sizes),
        mesh=mesh, in_specs=(spec, spec, spec), out_specs=spec, check_vma=False,
    )
```

```python
import functools
import math

import jax
import jax.numpy as jnp
from jax import lax
from jax.experimental import pallas as pl
from jax.experimental.pallas import tpu as pltpu
from jax.sharding import PartitionSpec as P

ITERS = 2
TWO_PI = 2.0 * math.pi
MESH = pl.DeviceIdType.MESH
LANES = 128
STRIP = 16


def cycles(change):
    return jnp.floor(change * (1.0 / TWO_PI) + 0.5)


def iota(shape, dim):
    return lax.broadcasted_iota(jnp.int32, shape, dim)


def total(values):
    return jnp.sum(values, axis=1, keepdims=True)


def shifted_in(values, first):
    lane = iota(values.shape, 1)
    return jnp.where(lane == 0, first, pltpu.roll(values, 1, 1))


def triangle(size, dim):
    ordered = iota((size, size), dim) <= iota((size, size), 1 - dim)
    return ordered.astype(jnp.float32).astype(jnp.bfloat16)


def line_counts(line, step):
    lane = iota(line.shape, 1)
    floors = jnp.where(lane == 0, 0.0, cycles(line - pltpu.roll(line, 1, 1)))
    floors = jnp.broadcast_to(floors, (16, line.shape[1]))
    upper, ones = triangle(step, 0), jnp.ones((step, step), jnp.bfloat16)
    earlier, counts = None, []
    for b in range(line.shape[1] // step):
        piece = floors[:, b * step : (b + 1) * step]
        count = jnp.dot(piece.astype(jnp.bfloat16), upper, preferred_element_type=jnp.float32)
        if b > 0:
            count = count + jnp.dot(
                earlier.astype(jnp.bfloat16), ones, preferred_element_type=jnp.float32
            )
        earlier = piece if b == 0 else earlier + piece
        counts.append(count[0:1, :])
    return jnp.concatenate(counts, axis=1)


def edge_kernel(
    names, sizes, rows_step, cols_step,
    wrapped, col_steps, row_steps,
    integ, offset,
    cells, left_out, up_out, right_in, below_in, corner_above, corner_left,
    last_row, end_lines, row_sums, floors, mine_out, every,
    load_sem, send_sem, recv_sem, gather_send, gather_recv, all_in,
):
    row_name, col_name = names
    grid_rows, grid_cols = sizes
    devices = grid_rows * grid_cols
    tile_rows, tile_cols = cells.shape
    my_row, my_col = lax.axis_index(row_name), lax.axis_index(col_name)
    me = my_row * grid_cols + my_col

    chunks = tile_rows // rows_step
    rest = pl.ds(LANES, tile_cols - LANES)
    regions = [(pl.ds(0, tile_rows), pl.ds(0, LANES)), (pl.ds(0, 16), rest)]
    for q in range(chunks):
        top = max(q * rows_step, 16)
        regions.append((pl.ds(top, (q + 1) * rows_step - top), rest))
    loads = []
    for k, (rows, cols) in enumerate(regions):
        loads.append(
            pltpu.make_async_copy(wrapped.at[0, rows, cols], cells.at[rows, cols], load_sem.at[k])
        )
        loads[-1].start()

    def row_place(p):
        return my_row, lax.rem(my_col + p, grid_cols)

    def col_place(p):
        return lax.rem(my_row + p, grid_rows), my_col

    def signal_all(semaphore, place, count):
        def signal(p, carry):
            pl.semaphore_signal(semaphore, inc=1, device_id=place(p), device_id_type=MESH)
            return carry

        lax.fori_loop(1, count, signal, 0)

    every[...] = jnp.zeros(every.shape, jnp.float32)

    barrier = pltpu.get_barrier_semaphore()
    signal_all(barrier, col_place, grid_rows)
    signal_all(barrier, row_place, grid_cols)

    with jax.named_scope("load_head"):
        loads[0].wait()
    with jax.named_scope("head"):
        for q in range(chunks):
            span = slice(q * rows_step, (q + 1) * rows_step)
            left_out[0:1, span] = cells[span, 0:LANES].T[0:1, :]
        left_out[1:2, :] = line_counts(left_out[0:1, :], rows_step)
    with jax.named_scope("load_top"):
        loads[1].wait()
    with jax.named_scope("first_row"):
        up_out[0:1, :] = cells[0:1, :]
        up_out[1:2, :] = line_counts(cells[0:1, :], cols_step)

    lane = iota((STRIP, LANES), 1)

    def strip(k, carry):
        rows = pl.ds(pl.multiple_of(k * STRIP, STRIP), STRIP)
        wrapped_around = cells[rows, 0:LANES]
        sums = jnp.zeros((STRIP, LANES), jnp.float32)
        for j in range(tile_cols // LANES):
            cols = slice(j * LANES, (j + 1) * LANES)
            here = cells[rows, cols]
            rolled = pltpu.roll(here, 1, 1)
            across = cycles(here - jnp.where(lane == 0, wrapped_around, rolled))
            wrapped_around = rolled
            floors[rows, cols] = across.astype(jnp.bfloat16)
            sums = sums + across
        row_sums[rows, :] = sums.astype(jnp.bfloat16)
        return carry

    per_chunk = rows_step // STRIP

    def set_floors(q):
        with jax.named_scope(f"load_{q}"):
            loads[q + 2].wait()
        with jax.named_scope(f"floors_{q}"):
            lax.fori_loop(q * per_chunk, (q + 1) * per_chunk, strip, 0, unroll=math.gcd(per_chunk, 8))

    early = chunks // 2
    for q in range(early):
        set_floors(q)

    with jax.named_scope("barrier"):
        pl.semaphore_wait(barrier, grid_rows + grid_cols - 2)
    corner = cells.at[pl.ds(tile_rows - 8, 8), pl.ds(tile_cols - LANES, LANES)]
    links = (
        (left_out, right_in, 0, -1, my_col > 0, my_col < grid_cols - 1),
        (up_out, below_in, -1, 0, my_row > 0, my_row < grid_rows - 1),
        (corner, corner_left, 0, 1, my_col < grid_cols - 1, my_col > 0),
        (corner, corner_above, 1, 0, my_row < grid_rows - 1, my_row > 0),
    )

    def link_copy(k, away):
        source, target, d_row, d_col, _, _ = links[k]
        place = (
            lax.rem(my_row + d_row * away + grid_rows, grid_rows),
            lax.rem(my_col + d_col * away + grid_cols, grid_cols),
        )
        return pltpu.make_async_remote_copy(
            src_ref=source, dst_ref=target, send_sem=send_sem.at[k], recv_sem=recv_sem.at[k],
            device_id=place, device_id_type=MESH,
        )

    def launch(k):
        sends, receives = links[k][4], links[k][5]

        @pl.when(sends)
        def _():
            link_copy(k, 1).start()

        @pl.when(jnp.logical_not(receives))
        def _():
            target = links[k][1]
            target[...] = jnp.zeros(target.shape, jnp.float32)

    launch(0)
    launch(1)
    signal_all(all_in, col_place, grid_rows)
    for q in range(early, chunks):
        set_floors(q)
        if q == chunks - 1:
            launch(2)
            launch(3)
    with jax.named_scope("ends"):
        ones = jnp.ones((16, LANES), jnp.bfloat16)
        for q in range(chunks):
            span = slice(q * rows_step, (q + 1) * rows_step)
            sums = lax.dot_general(
                ones, row_sums[span, :], (((1,), (1,)), ((), ())),
                preferred_element_type=jnp.float32,
            )
            end_lines[0:1, span] = left_out[1:2, span] + sums[0:1, :]
            end_lines[1:3, span] = cells[span, tile_cols - LANES :].T[LANES - 2 :, :]
    with jax.named_scope("last_row"):
        last_row[...] = left_out[1:2, tile_rows - 1 :] + line_counts(
            cells[tile_rows - 1 : tile_rows, :], cols_step
        )
    row_inner = cells[tile_rows - 2 : tile_rows - 1, :]
    row_outer = cells[tile_rows - 1 : tile_rows, :]

    with jax.named_scope("integrate"):
        upper, lower = triangle(cols_step, 0), triangle(rows_step, 1)
        down_carry = jnp.zeros((1, LANES), jnp.float32)
        for q in range(chunks):
            top = q * rows_step
            rows = pl.ds(top, rows_step)
            head = cells[rows, 0:LANES]
            above = cells[max(top - 1, 0) : max(top, 1), 0:LANES]
            before = jnp.where(iota(head.shape, 0) == 0, above, pltpu.roll(head, 1, 0))
            counts = down_carry + jnp.dot(
                lower, cycles(head - before).astype(jnp.bfloat16), preferred_element_type=jnp.float32
            )
            down_carry = counts[rows_step - 1 : rows_step, :]
            carry = counts[:, 0:1]
            for b in range(tile_cols // cols_step):
                cols = slice(b * cols_step, (b + 1) * cols_step)
                count = carry + jnp.dot(
                    floors[rows, cols], upper, preferred_element_type=jnp.float32
                )
                carry = count[:, cols_step - 1 : cols_step]
                integ[rows, cols] = cells[rows, cols] * (1.0 / TWO_PI) - count

    for k in range(4):

        with jax.named_scope(f"halo_{k}"):

            @pl.when(links[k][5])
            def _():
                link_copy(k, 1).wait_recv()

    def base(inner, outer, inner_before, outer_before, at_image_edge, first, count, beyond):
        over = cycles(outer - inner)
        over_before = shifted_in(over, cycles(outer_before - inner_before))
        along_outer = cycles(outer - shifted_in(outer, outer_before))
        along_inner = cycles(inner - shifted_in(inner, inner_before))
        charge = over_before + along_outer - over - along_inner
        charge = jnp.where((iota(charge.shape, 1) == 0) & at_image_edge, 0.0, charge)
        weight = 1.0 / (1.0 + jnp.abs(charge))
        jump = beyond - count - cycles(first - outer)
        return total(weight * jump) / total(weight)

    across_base = base(
        end_lines[1:2, :], end_lines[2:3, :],
        corner_above[7:8, LANES - 2 : LANES - 1], corner_above[7:8, LANES - 1 : LANES],
        my_row == 0, right_in[0:1, :], end_lines[0:1, :], right_in[1:2, :],
    ) + col_steps[0].astype(jnp.float32)
    down_base = base(
        row_inner, row_outer,
        corner_left[6:7, LANES - 1 : LANES], corner_left[7:8, LANES - 1 : LANES],
        my_col == 0, below_in[0:1, :], last_row[...], below_in[1:2, :],
    ) + row_steps[0].astype(jnp.float32)
    slot = iota((1, LANES), 1)
    mine_out[...] = jnp.where(
        slot == my_col, across_base, jnp.where(slot == grid_cols + my_col, down_base, 0.0)
    )

    def gather_copy(row, col, owner):
        peer = row * grid_cols + col
        return pltpu.make_async_remote_copy(
            src_ref=mine_out, dst_ref=every.at[owner], send_sem=gather_send.at[peer],
            recv_sem=gather_recv.at[owner], device_id=(row, col), device_id_type=MESH,
        )

    def span(low, high, act):
        def step(k, carry):
            act(k)
            return carry

        lax.fori_loop(low, high, step, 0)

    def each_target(act):
        first_row = jnp.where(my_row == 0, 1, jnp.where(my_col == 0, my_row + 1, grid_rows))
        span(first_row, grid_rows, lambda r: span(my_col + 1, grid_cols, lambda c: act(r, c)))
        span(my_col + 1, grid_cols, lambda c: act(my_row, c))
        span(my_row + 1, grid_rows, lambda r: act(r, my_col))

    def each_source(act):
        span(0, my_col, lambda c: act(my_row, c))
        span(0, my_row, lambda r: act(r, my_col))
        span(0, jnp.where(my_row > 0, my_col, 0), lambda c: act(0, c))
        span(1, jnp.where(my_col > 0, my_row, 0), lambda r: act(r, 0))

    with jax.named_scope("all_in"):
        pl.semaphore_wait(all_in, grid_rows - 1)
    with jax.named_scope("tell"):
        each_target(lambda r, c: gather_copy(r, c, me).start())
    with jax.named_scope("sent"):
        for k in range(4):

            @pl.when(links[k][4])
            def _():
                link_copy(k, 1).wait_send()

    with jax.named_scope("hear"):
        each_source(lambda r, c: gather_copy(r, c, r * grid_cols + c).wait_recv())

    padded = -(-grid_rows // 8) * 8
    tile_row = iota((padded, LANES), 0)
    tile_lane = iota((padded, LANES), 1)
    grid = jnp.zeros((padded, LANES), jnp.float32)
    for r in range(grid_rows):
        line = every[r * grid_cols]
        for c in range(1, grid_cols):
            line = line + every[r * grid_cols + c]
        grid = jnp.where(tile_row == r, line, grid)
    def summed(mask):
        picked = jnp.where(mask, grid, 0.0)
        return jnp.sum(jnp.sum(picked, axis=0, keepdims=True), axis=1, keepdims=True)

    earlier_cols = tile_lane < my_col
    across_here = summed((tile_row == my_row) & earlier_cols)
    across_top = summed((tile_row == 0) & earlier_cols)
    down_here = summed((tile_row < my_row) & (tile_lane == grid_cols + my_col))
    down_left = summed((tile_row < my_row) & (tile_lane == grid_cols))
    here = left = top = origin = jnp.zeros((1, 1), jnp.float32)
    for sweep in range(ITERS):
        prefix_across = across_here + (left - here)
        prefix_across_top = across_top + (origin - top)
        prefix_down = down_here + (top - here)
        prefix_down_left = down_left + (origin - left)
        here = here + 0.5 * (prefix_across + prefix_across_top + prefix_down + prefix_down_left)
        left = left + prefix_down_left
        top = top + prefix_across_top
    offset[...] = jnp.broadcast_to(here, offset.shape)
    each_target(lambda r, c: gather_copy(r, c, me).wait_send())


def place_kernel(integ, offset, out, ready, sems):
    parts = sems.shape[0]
    step = integ.shape[0] // parts
    shift = offset[0:1, 0:1]
    copies = []
    for q in range(parts):
        rows = pl.ds(q * step, step)
        ready[rows, :] = integ[rows, :] + shift
        copy = pltpu.make_async_copy(ready.at[rows], out.at[rows], sems.at[q])
        copy.start()
        copies.append(copy)
    for copy in copies:
        copy.wait()


def on_device(names, sizes, wrapped, col_steps, row_steps):
    frames, tile_rows, tile_cols = wrapped.shape
    devices = sizes[0] * sizes[1]
    rows_step = math.gcd(tile_rows, 256)
    cols_step = math.gcd(tile_cols, 256)
    f32 = jnp.float32
    call = pl.pallas_call(
        functools.partial(edge_kernel, names, sizes, rows_step, cols_step),
        out_shape=(
            pltpu.VMEM((tile_rows, tile_cols), f32),
            pltpu.VMEM((8, LANES), f32),
        ),
        in_specs=[
            pl.BlockSpec(memory_space=pltpu.HBM),
            pl.BlockSpec(memory_space=pltpu.VMEM),
            pl.BlockSpec(memory_space=pltpu.VMEM),
        ],
        out_specs=(
            pl.BlockSpec(memory_space=pltpu.VMEM),
            pl.BlockSpec(memory_space=pltpu.VMEM),
        ),
        scratch_shapes=[
            pltpu.VMEM((tile_rows, tile_cols), f32),
            pltpu.VMEM((2, tile_rows), f32),
            pltpu.VMEM((2, tile_cols), f32),
            pltpu.VMEM((2, tile_rows), f32),
            pltpu.VMEM((2, tile_cols), f32),
            pltpu.VMEM((8, LANES), f32),
            pltpu.VMEM((8, LANES), f32),
            pltpu.VMEM((1, tile_cols), f32),
            pltpu.VMEM((3, tile_rows), f32),
            pltpu.VMEM((tile_rows, LANES), jnp.bfloat16),
            pltpu.VMEM((tile_rows, tile_cols), jnp.bfloat16),
            pltpu.VMEM((1, LANES), f32),
            pltpu.VMEM((devices, 1, LANES), f32),
            pltpu.SemaphoreType.DMA((tile_rows // rows_step + 2,)),
            pltpu.SemaphoreType.DMA((4,)),
            pltpu.SemaphoreType.DMA((4,)),
            pltpu.SemaphoreType.DMA((devices,)),
            pltpu.SemaphoreType.DMA((devices,)),
            pltpu.SemaphoreType.REGULAR,
        ],
        compiler_params=pltpu.CompilerParams(
            collective_id=0, has_side_effects=True, vmem_limit_bytes=57 * 1024 * 1024
        ),
    )
    parts = math.gcd(tile_rows // 8, 16)
    place = pl.pallas_call(
        place_kernel,
        out_shape=jax.ShapeDtypeStruct((tile_rows, tile_cols), f32),
        in_specs=[pl.BlockSpec(memory_space=pltpu.VMEM), pl.BlockSpec(memory_space=pltpu.VMEM)],
        out_specs=pl.BlockSpec(memory_space=pltpu.HBM),
        scratch_shapes=[
            pltpu.VMEM((tile_rows, tile_cols), f32),
            pltpu.SemaphoreType.DMA((parts,)),
        ],
        compiler_params=pltpu.CompilerParams(vmem_limit_bytes=24 * 1024 * 1024),
    )
    outs = [
        place(*call(wrapped[f : f + 1], col_steps[f : f + 1], row_steps[f : f + 1]))
        for f in range(frames)
    ]
    return jnp.stack(outs)


def solution(mesh):
    spec = P(None, "row", "col")
    sizes = (mesh.shape["row"], mesh.shape["col"])
    return jax.shard_map(
        functools.partial(on_device, ("row", "col"), sizes),
        mesh=mesh, in_specs=(spec, spec, spec), out_specs=spec, check_vma=False,
    )
```

```python
import functools
import math

import jax
import jax.numpy as jnp
from jax import lax
from jax.experimental import pallas as pl
from jax.experimental.pallas import tpu as pltpu
from jax.sharding import PartitionSpec as P

ITERS = 2
TWO_PI = 2.0 * math.pi
MESH = pl.DeviceIdType.MESH
LANES = 128
STRIP = 16


def cycles(change):
    return jnp.floor(change * (1.0 / TWO_PI) + 0.5)


def iota(shape, dim):
    return lax.broadcasted_iota(jnp.int32, shape, dim)


def total(values):
    return jnp.sum(values, axis=1, keepdims=True)


def shifted_in(values, first):
    lane = iota(values.shape, 1)
    return jnp.where(lane == 0, first, pltpu.roll(values, 1, 1))


def triangle(size, dim):
    ordered = iota((size, size), dim) <= iota((size, size), 1 - dim)
    return ordered.astype(jnp.float32).astype(jnp.bfloat16)


def line_counts(line, step):
    lane = iota(line.shape, 1)
    floors = jnp.where(lane == 0, 0.0, cycles(line - pltpu.roll(line, 1, 1)))
    floors = jnp.broadcast_to(floors, (16, line.shape[1]))
    upper, ones = triangle(step, 0), jnp.ones((step, step), jnp.bfloat16)
    earlier, counts = None, []
    for b in range(line.shape[1] // step):
        piece = floors[:, b * step : (b + 1) * step]
        count = jnp.dot(piece.astype(jnp.bfloat16), upper, preferred_element_type=jnp.float32)
        if b > 0:
            count = count + jnp.dot(
                earlier.astype(jnp.bfloat16), ones, preferred_element_type=jnp.float32
            )
        earlier = piece if b == 0 else earlier + piece
        counts.append(count[0:1, :])
    return jnp.concatenate(counts, axis=1)


def edge_kernel(
    names, sizes, rows_step, cols_step,
    wrapped, col_steps, row_steps,
    integ, offset,
    cells, left_out, up_out, right_in, below_in, corner_above, corner_left,
    last_row, end_lines, row_sums, floors, mine_out, every,
    load_sem, send_sem, recv_sem, gather_send, gather_recv, all_in,
):
    row_name, col_name = names
    grid_rows, grid_cols = sizes
    devices = grid_rows * grid_cols
    tile_rows, tile_cols = cells.shape
    my_row, my_col = lax.axis_index(row_name), lax.axis_index(col_name)
    me = my_row * grid_cols + my_col

    chunks = tile_rows // rows_step
    rest = pl.ds(LANES, tile_cols - LANES)
    regions = [(pl.ds(0, tile_rows), pl.ds(0, LANES)), (pl.ds(0, 16), rest)]
    for q in range(chunks):
        top = max(q * rows_step, 16)
        regions.append((pl.ds(top, (q + 1) * rows_step - top), rest))
    loads = []
    for k, (rows, cols) in enumerate(regions):
        loads.append(
            pltpu.make_async_copy(wrapped.at[0, rows, cols], cells.at[rows, cols], load_sem.at[k])
        )
        loads[-1].start()

    def row_place(p):
        return my_row, lax.rem(my_col + p, grid_cols)

    def col_place(p):
        return lax.rem(my_row + p, grid_rows), my_col

    def signal_all(semaphore, place, count):
        def signal(p, carry):
            pl.semaphore_signal(semaphore, inc=1, device_id=place(p), device_id_type=MESH)
            return carry

        lax.fori_loop(1, count, signal, 0)

    every[...] = jnp.zeros(every.shape, jnp.float32)

    barrier = pltpu.get_barrier_semaphore()
    signal_all(barrier, col_place, grid_rows)
    signal_all(barrier, row_place, grid_cols)

    with jax.named_scope("load_head"):
        loads[0].wait()
    with jax.named_scope("head"):
        for q in range(chunks):
            span = slice(q * rows_step, (q + 1) * rows_step)
            left_out[0:1, span] = cells[span, 0:LANES].T[0:1, :]
        left_out[1:2, :] = line_counts(left_out[0:1, :], rows_step)
    with jax.named_scope("load_top"):
        loads[1].wait()
    with jax.named_scope("first_row"):
        up_out[0:1, :] = cells[0:1, :]
        up_out[1:2, :] = line_counts(cells[0:1, :], cols_step)

    lane = iota((STRIP, LANES), 1)

    def strip(k, carry):
        rows = pl.ds(pl.multiple_of(k * STRIP, STRIP), STRIP)
        wrapped_around = cells[rows, 0:LANES]
        sums = jnp.zeros((STRIP, LANES), jnp.float32)
        for j in range(tile_cols // LANES):
            cols = slice(j * LANES, (j + 1) * LANES)
            here = cells[rows, cols]
            rolled = pltpu.roll(here, 1, 1)
            across = cycles(here - jnp.where(lane == 0, wrapped_around, rolled))
            wrapped_around = rolled
            floors[rows, cols] = across.astype(jnp.bfloat16)
            sums = sums + across
        row_sums[rows, :] = sums.astype(jnp.bfloat16)
        return carry

    per_chunk = rows_step // STRIP

    def set_floors(q):
        with jax.named_scope(f"floors_{q}"):
            lax.fori_loop(q * per_chunk, (q + 1) * per_chunk, strip, 0, unroll=math.gcd(per_chunk, 8))

    early = chunks // 2
    for q in range(early):
        loads[q + 2].wait()
        set_floors(q)

    with jax.named_scope("barrier"):
        pl.semaphore_wait(barrier, grid_rows + grid_cols - 2)
    corner = cells.at[pl.ds(tile_rows - 8, 8), pl.ds(tile_cols - LANES, LANES)]
    links = (
        (left_out, right_in, 0, -1, my_col > 0, my_col < grid_cols - 1),
        (up_out, below_in, -1, 0, my_row > 0, my_row < grid_rows - 1),
        (corner, corner_left, 0, 1, my_col < grid_cols - 1, my_col > 0),
        (corner, corner_above, 1, 0, my_row < grid_rows - 1, my_row > 0),
    )

    def link_copy(k, away):
        source, target, d_row, d_col, _, _ = links[k]
        place = (
            lax.rem(my_row + d_row * away + grid_rows, grid_rows),
            lax.rem(my_col + d_col * away + grid_cols, grid_cols),
        )
        return pltpu.make_async_remote_copy(
            src_ref=source, dst_ref=target, send_sem=send_sem.at[k], recv_sem=recv_sem.at[k],
            device_id=place, device_id_type=MESH,
        )

    def launch(k):
        sends, receives = links[k][4], links[k][5]

        @pl.when(sends)
        def _():
            link_copy(k, 1).start()

        @pl.when(jnp.logical_not(receives))
        def _():
            target = links[k][1]
            target[...] = jnp.zeros(target.shape, jnp.float32)

    launch(0)
    launch(1)
    signal_all(all_in, col_place, grid_rows)
    for q in range(early, chunks):
        loads[q + 2].wait()
    launch(3)
    launch(2)
    for q in range(early, chunks):
        set_floors(q)
    with jax.named_scope("ends"):
        ones = jnp.ones((16, LANES), jnp.bfloat16)
        for q in range(chunks):
            span = slice(q * rows_step, (q + 1) * rows_step)
            sums = lax.dot_general(
                ones, row_sums[span, :], (((1,), (1,)), ((), ())),
                preferred_element_type=jnp.float32,
            )
            end_lines[0:1, span] = left_out[1:2, span] + sums[0:1, :]
            end_lines[1:3, span] = cells[span, tile_cols - LANES :].T[LANES - 2 :, :]
    with jax.named_scope("last_row"):
        last_row[...] = left_out[1:2, tile_rows - 1 :] + line_counts(
            cells[tile_rows - 1 : tile_rows, :], cols_step
        )
    row_inner = cells[tile_rows - 2 : tile_rows - 1, :]
    row_outer = cells[tile_rows - 1 : tile_rows, :]

    with jax.named_scope("integrate"):
        upper, lower = triangle(cols_step, 0), triangle(rows_step, 1)
        down_carry = jnp.zeros((1, LANES), jnp.float32)
        for q in range(chunks):
            top = q * rows_step
            rows = pl.ds(top, rows_step)
            head = cells[rows, 0:LANES]
            above = cells[max(top - 1, 0) : max(top, 1), 0:LANES]
            before = jnp.where(iota(head.shape, 0) == 0, above, pltpu.roll(head, 1, 0))
            counts = down_carry + jnp.dot(
                lower, cycles(head - before).astype(jnp.bfloat16), preferred_element_type=jnp.float32
            )
            down_carry = counts[rows_step - 1 : rows_step, :]
            carry = counts[:, 0:1]
            for b in range(tile_cols // cols_step):
                cols = slice(b * cols_step, (b + 1) * cols_step)
                count = carry + jnp.dot(
                    floors[rows, cols], upper, preferred_element_type=jnp.float32
                )
                carry = count[:, cols_step - 1 : cols_step]
                integ[rows, cols] = cells[rows, cols] * (1.0 / TWO_PI) - count

    for k in range(4):

        with jax.named_scope(f"halo_{k}"):

            @pl.when(links[k][5])
            def _():
                link_copy(k, 1).wait_recv()

    def base(inner, outer, inner_before, outer_before, at_image_edge, first, count, beyond):
        over = cycles(outer - inner)
        over_before = shifted_in(over, cycles(outer_before - inner_before))
        along_outer = cycles(outer - shifted_in(outer, outer_before))
        along_inner = cycles(inner - shifted_in(inner, inner_before))
        charge = over_before + along_outer - over - along_inner
        charge = jnp.where((iota(charge.shape, 1) == 0) & at_image_edge, 0.0, charge)
        weight = 1.0 / (1.0 + jnp.abs(charge))
        jump = beyond - count - cycles(first - outer)
        return total(weight * jump) / total(weight)

    across_base = base(
        end_lines[1:2, :], end_lines[2:3, :],
        corner_above[7:8, LANES - 2 : LANES - 1], corner_above[7:8, LANES - 1 : LANES],
        my_row == 0, right_in[0:1, :], end_lines[0:1, :], right_in[1:2, :],
    ) + col_steps[0].astype(jnp.float32)
    down_base = base(
        row_inner, row_outer,
        corner_left[6:7, LANES - 1 : LANES], corner_left[7:8, LANES - 1 : LANES],
        my_col == 0, below_in[0:1, :], last_row[...], below_in[1:2, :],
    ) + row_steps[0].astype(jnp.float32)
    slot = iota((1, LANES), 1)
    mine_out[...] = jnp.where(
        slot == my_col, across_base, jnp.where(slot == grid_cols + my_col, down_base, 0.0)
    )

    def gather_copy(row, col, owner):
        peer = row * grid_cols + col
        return pltpu.make_async_remote_copy(
            src_ref=mine_out, dst_ref=every.at[owner], send_sem=gather_send.at[peer],
            recv_sem=gather_recv.at[owner], device_id=(row, col), device_id_type=MESH,
        )

    def span(low, high, act):
        def step(k, carry):
            act(k)
            return carry

        lax.fori_loop(low, high, step, 0)

    def each_target(act):
        first_row = jnp.where(my_row == 0, 1, jnp.where(my_col == 0, my_row + 1, grid_rows))
        span(first_row, grid_rows, lambda r: span(my_col + 1, grid_cols, lambda c: act(r, c)))
        span(my_col + 1, grid_cols, lambda c: act(my_row, c))
        span(my_row + 1, grid_rows, lambda r: act(r, my_col))

    def each_source(act):
        span(0, my_col, lambda c: act(my_row, c))
        span(0, my_row, lambda r: act(r, my_col))
        span(0, jnp.where(my_row > 0, my_col, 0), lambda c: act(0, c))
        span(1, jnp.where(my_col > 0, my_row, 0), lambda r: act(r, 0))

    with jax.named_scope("all_in"):
        pl.semaphore_wait(all_in, grid_rows - 1)
    with jax.named_scope("tell"):
        each_target(lambda r, c: gather_copy(r, c, me).start())
    with jax.named_scope("sent"):
        for k in range(4):

            @pl.when(links[k][4])
            def _():
                link_copy(k, 1).wait_send()

    with jax.named_scope("hear"):
        each_source(lambda r, c: gather_copy(r, c, r * grid_cols + c).wait_recv())

    padded = -(-grid_rows // 8) * 8
    tile_row = iota((padded, LANES), 0)
    tile_lane = iota((padded, LANES), 1)
    grid = jnp.zeros((padded, LANES), jnp.float32)
    for r in range(grid_rows):
        line = every[r * grid_cols]
        for c in range(1, grid_cols):
            line = line + every[r * grid_cols + c]
        grid = jnp.where(tile_row == r, line, grid)
    def summed(mask):
        picked = jnp.where(mask, grid, 0.0)
        return jnp.sum(jnp.sum(picked, axis=0, keepdims=True), axis=1, keepdims=True)

    earlier_cols = tile_lane < my_col
    across_here = summed((tile_row == my_row) & earlier_cols)
    across_top = summed((tile_row == 0) & earlier_cols)
    down_here = summed((tile_row < my_row) & (tile_lane == grid_cols + my_col))
    down_left = summed((tile_row < my_row) & (tile_lane == grid_cols))
    here = left = top = origin = jnp.zeros((1, 1), jnp.float32)
    for sweep in range(ITERS):
        prefix_across = across_here + (left - here)
        prefix_across_top = across_top + (origin - top)
        prefix_down = down_here + (top - here)
        prefix_down_left = down_left + (origin - left)
        here = here + 0.5 * (prefix_across + prefix_across_top + prefix_down + prefix_down_left)
        left = left + prefix_down_left
        top = top + prefix_across_top
    offset[...] = jnp.broadcast_to(here, offset.shape)
    each_target(lambda r, c: gather_copy(r, c, me).wait_send())


def place_kernel(integ, offset, out, ready, sems):
    parts = sems.shape[0]
    step = integ.shape[0] // parts
    shift = offset[0:1, 0:1]
    copies = []
    for q in range(parts):
        rows = pl.ds(q * step, step)
        ready[rows, :] = integ[rows, :] + shift
        copy = pltpu.make_async_copy(ready.at[rows], out.at[rows], sems.at[q])
        copy.start()
        copies.append(copy)
    for copy in copies:
        copy.wait()


def on_device(names, sizes, wrapped, col_steps, row_steps):
    frames, tile_rows, tile_cols = wrapped.shape
    devices = sizes[0] * sizes[1]
    rows_step = math.gcd(tile_rows, 256)
    cols_step = math.gcd(tile_cols, 256)
    f32 = jnp.float32
    call = pl.pallas_call(
        functools.partial(edge_kernel, names, sizes, rows_step, cols_step),
        out_shape=(
            pltpu.VMEM((tile_rows, tile_cols), f32),
            pltpu.VMEM((8, LANES), f32),
        ),
        in_specs=[
            pl.BlockSpec(memory_space=pltpu.HBM),
            pl.BlockSpec(memory_space=pltpu.VMEM),
            pl.BlockSpec(memory_space=pltpu.VMEM),
        ],
        out_specs=(
            pl.BlockSpec(memory_space=pltpu.VMEM),
            pl.BlockSpec(memory_space=pltpu.VMEM),
        ),
        scratch_shapes=[
            pltpu.VMEM((tile_rows, tile_cols), f32),
            pltpu.VMEM((2, tile_rows), f32),
            pltpu.VMEM((2, tile_cols), f32),
            pltpu.VMEM((2, tile_rows), f32),
            pltpu.VMEM((2, tile_cols), f32),
            pltpu.VMEM((8, LANES), f32),
            pltpu.VMEM((8, LANES), f32),
            pltpu.VMEM((1, tile_cols), f32),
            pltpu.VMEM((3, tile_rows), f32),
            pltpu.VMEM((tile_rows, LANES), jnp.bfloat16),
            pltpu.VMEM((tile_rows, tile_cols), jnp.bfloat16),
            pltpu.VMEM((1, LANES), f32),
            pltpu.VMEM((devices, 1, LANES), f32),
            pltpu.SemaphoreType.DMA((tile_rows // rows_step + 2,)),
            pltpu.SemaphoreType.DMA((4,)),
            pltpu.SemaphoreType.DMA((4,)),
            pltpu.SemaphoreType.DMA((devices,)),
            pltpu.SemaphoreType.DMA((devices,)),
            pltpu.SemaphoreType.REGULAR,
        ],
        compiler_params=pltpu.CompilerParams(
            collective_id=0, has_side_effects=True, vmem_limit_bytes=57 * 1024 * 1024
        ),
    )
    parts = math.gcd(tile_rows // 8, 16)
    place = pl.pallas_call(
        place_kernel,
        out_shape=jax.ShapeDtypeStruct((tile_rows, tile_cols), f32),
        in_specs=[pl.BlockSpec(memory_space=pltpu.VMEM), pl.BlockSpec(memory_space=pltpu.VMEM)],
        out_specs=pl.BlockSpec(memory_space=pltpu.HBM),
        scratch_shapes=[
            pltpu.VMEM((tile_rows, tile_cols), f32),
            pltpu.SemaphoreType.DMA((parts,)),
        ],
        compiler_params=pltpu.CompilerParams(vmem_limit_bytes=24 * 1024 * 1024),
    )
    outs = [
        place(*call(wrapped[f : f + 1], col_steps[f : f + 1], row_steps[f : f + 1]))
        for f in range(frames)
    ]
    return jnp.stack(outs)


def solution(mesh):
    spec = P(None, "row", "col")
    sizes = (mesh.shape["row"], mesh.shape["col"])
    return jax.shard_map(
        functools.partial(on_device, ("row", "col"), sizes),
        mesh=mesh, in_specs=(spec, spec, spec), out_specs=spec, check_vma=False,
    )
```
